32 devices in a mesh: gx: 4 (over y, x), gy: 4 (over z), gz: 2 (over core).
Axes of the slice: x: 2, y: 2, z: 4, core: 2. Of those that a mesh axis runs over, the one named last changes fastest.
Arguments:
- right_side: float32 [64, 256, 1024], P('gx', 'gy', 'gz'), may hold values from -24 to 24
- reaction: float32 [64, 256, 1024], P('gx', 'gy', 'gz'), may hold values from 0.5 to 2
- velocity: float32 [3, 64, 256, 1024], P(None, 'gx', 'gy', 'gz'), may hold values from -0.5 to 0.5
Outputs:
- solution: float32 [64, 256, 1024], P('gx', 'gy', 'gz')
- residual: float32 [64, 256, 1024], P('gx', 'gy', 'gz')
- residual_norm: float32 [], replicated
The draws below stay inside these ranges and needn't reach their ends.
All inputs are finite; a program needn't handle non-finite values.
Results may differ from the reference program's by a relative error of at most 0.00002.
Values sent between devices are 32-bit elements; how exact they have to be, the bound alone decides.
A program may use at most 128 MiB of HBM per device.

```python
import math
import jax
import jax.numpy as jnp

ITERS = 5
NX = 64
NY = 256
NZ = 1024


def draw_right_side(key, part):
    noise_key = jax.random.fold_in(jax.random.fold_in(key, 11), 0)
    ramp = 1.0 + 2.0 * jnp.arange(NX, dtype=jnp.float32)[:, None, None] / max(NX - 1, 1)
    values = ramp * jnp.clip(jax.random.normal(noise_key, (NX, NY, NZ), jnp.float32), -6.0, 6.0)
    return values.astype(jnp.float32)


def block_levels(own_key, extent, shards, least, top_value):
    def one(position, blocks):
        steps = jax.random.uniform(jax.random.fold_in(jax.random.fold_in(own_key, 6), position), (blocks,), jnp.float32, least / len(shards), top_value / len(shards))
        return jnp.repeat(jnp.exp(steps), extent[position] // blocks).reshape((-1,) + (1,) * (len(extent) - position - 1))

    loudness = one(*shards[0])
    for cut in shards[1:]:
        loudness = loudness * one(*cut)
    return loudness


def setup_inputs(seed: int = 0) -> dict:
    arg_keys = jax.random.split(jax.random.key(seed), 4)
    return {
        "right_side": draw_right_side(jax.random.fold_in(arg_keys[3], 71), 0),
        "reaction": jnp.clip(jnp.exp(math.log(2.0) - 1.3862944 * jax.random.uniform(arg_keys[1], (NX, NY, NZ), jnp.float32) ** block_levels(arg_keys[1], (NX, NY, NZ), ((0, 4), (1, 4), (2, 2)), -0.2, 0.2)), 0.5, 2.0),
        "velocity": jnp.clip(jax.random.uniform(arg_keys[2], (3, NX, NY, NZ), jnp.float32, -0.5, 0.5) * block_levels(arg_keys[2], (3, NX, NY, NZ), ((1, 4), (2, 4), (3, 2)), -0.4, 0.0), -0.5, 0.5),
    }


centre = 7.25
half_width = 6.75

def chebyshev_weights(count):
    ratio_value = centre / half_width
    weights = [1.0 / ratio_value]
    for iteration in range(count):
        weights.append(1.0 / (2.0 * ratio_value - weights[-1]))
    return weights

def combine(middle, plus_x, minus_x, plus_y, minus_y, plus_z, minus_z, reaction, velocity):
    beside = (1.0 - velocity[0]) * plus_x + (1.0 + velocity[0]) * minus_x
    beside = beside + (1.0 - velocity[1]) * plus_y + (1.0 + velocity[1]) * minus_y
    beside = beside + (1.0 - velocity[2]) * plus_z + (1.0 + velocity[2]) * minus_z
    return (6.0 + reaction) * middle - beside

def operate(values, reaction, velocity):
    plus_x = jnp.roll(values, -1, 0)
    minus_x = jnp.roll(values, 1, 0)
    padded = jnp.pad(values, ((0, 0), (1, 1), (1, 1)))
    return combine(values, plus_x, minus_x, padded[:, 2:, 1:-1], padded[:, :-2, 1:-1], padded[:, 1:-1, 2:], padded[:, 1:-1, :-2], reaction, velocity)

def reference(right_side, reaction, velocity):
    weights = chebyshev_weights(ITERS)
    solution = jnp.zeros_like(right_side)
    residual = right_side
    direction = right_side / centre
    for iteration in range(ITERS):
        applied = operate(direction, reaction, velocity)
        solution = solution + direction
        residual = residual - applied
        if iteration + 1 < ITERS:
            direction = weights[iteration + 1] * weights[iteration] * direction + 2.0 * weights[iteration + 1] / half_width * residual
    residual_norm = jnp.sqrt(jnp.sum(residual * residual) / (NX * NY * NZ) + 1e-06)
    return (solution, residual, residual_norm)
```

```python
import functools

import jax
import jax.numpy as jnp
from jax import lax
from jax.experimental import pallas as pl
from jax.experimental.pallas import tpu as pltpu
from jax.sharding import PartitionSpec as P

ITERS = 5
CHUNKS = 4
ROWS = 8

centre = 7.25
half_width = 6.75

AXES = ("gx", "gy", "gz")
PY, PZ = 8, 128
LOW, HIGH, INNER = 0, 1, 2


def chebyshev_weights(count):
    ratio_value = centre / half_width
    weights = [1.0 / ratio_value]
    for iteration in range(count):
        weights.append(1.0 / (2.0 * ratio_value - weights[-1]))
    return weights


def kernel(
    sizes,
    rhs,
    reaction,
    velocity,
    sol,
    res,
    norm,
    d,
    reac,
    vel,
    ysend,
    yrecv,
    part,
    load_sem,
    xs_sem,
    xr_sem,
    ys_sem,
    yr_sem,
    zs_sem,
    zr_sem,
    ps_sem,
    pr_sem,
):
    nx, ny, nz = rhs.shape
    weights = chebyshev_weights(ITERS)
    me = [lax.axis_index(a) for a in AXES]
    mid_y = pl.ds(PY, ny)
    mid_z = pl.ds(PZ, nz)
    chunk = ny // CHUNKS

    load_rhs = pltpu.make_async_copy(
        rhs, d.at[0, pl.ds(1, nx), mid_y, mid_z], load_sem.at[0]
    )
    load_rhs.start()
    loads = [pltpu.make_async_copy(reaction, reac, load_sem.at[1])] + [
        pltpu.make_async_copy(velocity.at[i], vel.at[i], load_sem.at[2 + i])
        for i in range(3)
    ]
    for copy in loads:
        copy.start()

    barrier = pltpu.get_barrier_semaphore()
    for a, n, i in zip(AXES, sizes, me):
        for p in range(1, n):
            pl.semaphore_signal(
                barrier,
                inc=1,
                device_id={a: lax.rem(i + p, n)},
                device_id_type=pl.DeviceIdType.MESH,
            )

    for side, at_edge in ((LOW, me[1] == 0), (HIGH, me[1] == sizes[1] - 1)):
        @pl.when(at_edge)
        def _(side=side):
            for slot in range(2):
                yrecv[slot, side] = jnp.zeros((nx, 1, nz), jnp.float32)

    for first, at_edge in ((0, me[2] == 0), (PZ + nz, me[2] == sizes[2] - 1)):
        @pl.when(at_edge)
        def _(first=first):
            def clear(x, carry):
                for slot in range(2):
                    d[slot, x, pl.ds(PY, ny), pl.ds(first, PZ)] = jnp.zeros(
                        (ny, PZ), jnp.float32
                    )
                return carry

            lax.fori_loop(1, nx + 1, clear, 0)

    pl.semaphore_wait(barrier, sum(n - 1 for n in sizes))

    def remote(src, dst, send, recv, axis, target):
        return pltpu.make_async_remote_copy(
            src_ref=src,
            dst_ref=dst,
            send_sem=send,
            recv_sem=recv,
            device_id={AXES[axis]: target},
            device_id_type=pl.DeviceIdType.MESH,
        )

    def x_copy(slot, side, c, source=None):
        n = sizes[0]
        rows = pl.ds(PY + c * chunk, chunk)
        plane, land, target = (
            (nx, 0, lax.rem(me[0] + 1, n))
            if side == LOW
            else (1, nx + 1, lax.rem(me[0] + n - 1, n))
        )
        if source is None:
            src = d.at[slot, plane, rows, mid_z]
        else:
            src = source.at[plane - 1, pl.ds(c * chunk, chunk), :]
        return remote(
            src,
            d.at[slot, land, rows, mid_z],
            xs_sem.at[slot, side, c],
            xr_sem.at[slot, side, c],
            0,
            target,
        )

    def span(group):
        return {LOW: (0, 1), HIGH: (nx - 1, 1), INNER: (1, nx - 2)}[group]

    def target_of(axis, side):
        n = sizes[axis]
        step = 1 if side == LOW else n - 1
        return lax.rem(me[axis] + step, n)

    def sends(axis, side):
        return me[axis] < sizes[axis] - 1 if side == LOW else me[axis] > 0

    def receives(axis, side):
        return me[axis] > 0 if side == LOW else me[axis] < sizes[axis] - 1

    def y_copy(slot, side, group):
        x = pl.ds(*span(group))
        return remote(
            ysend.at[slot, side, x],
            yrecv.at[slot, side, x],
            ys_sem.at[slot, side, group],
            yr_sem.at[slot, side, group],
            1,
            target_of(1, side),
        )

    def z_copy(slot, side, group):
        first, count = span(group)
        x = pl.ds(first + 1, count)
        source, land = (nz, 0) if side == LOW else (PZ, PZ + nz)
        return remote(
            d.at[slot, x, mid_y, pl.ds(source, PZ)],
            d.at[slot, x, mid_y, pl.ds(land, PZ)],
            zs_sem.at[slot, side, group],
            zr_sem.at[slot, side, group],
            2,
            target_of(2, side),
        )

    def open_each(slot, groups, act):
        for group in groups:
            for axis, copy in ((2, z_copy), (1, y_copy)):
                for side in (LOW, HIGH):
                    rule = receives if act == "wait_recv" else sends

                    @pl.when(rule(axis, side))
                    def _(copy=copy, side=side, group=group):
                        getattr(copy(slot, side, group), act)()

    def pack(slot, x):
        ysend[slot, LOW, x - 1] = d[slot, x, pl.ds(PY + ny - 1, 1), mid_z]
        ysend[slot, HIGH, x - 1] = d[slot, x, pl.ds(PY, 1), mid_z]

    def unpack(slot, x):
        d[slot, x, pl.ds(PY - 1, 1), mid_z] = yrecv[slot, LOW, x - 1]
        d[slot, x, pl.ds(PY + ny, 1), mid_z] = yrecv[slot, HIGH, x - 1]

    def block(k, x, y):
        slot, other = k % 2, (k + 1) % 2
        here = (x - 1, pl.ds(y, ROWS), slice(None))
        rows = pl.ds(PY + y, ROWS)
        mid = d[slot, x, rows, mid_z]
        px = d[slot, x + 1, rows, mid_z]
        mx = d[slot, x - 1, rows, mid_z]
        py = d[slot, x, pl.ds(PY + y + 1, ROWS), mid_z]
        my = d[slot, x, pl.ds(PY + y - 1, ROWS), mid_z]
        wide = nz + PZ
        pz = pltpu.roll(d[slot, x, rows, pl.ds(PZ, wide)], wide - 1, 1)[:, :nz]
        mz = pltpu.roll(d[slot, x, rows, pl.ds(0, wide)], 1, 1)[:, PZ:]
        beside = ((px + mx) + (py + my)) + (pz + mz)
        skew = vel[0, *here] * (px - mx) + vel[1, *here] * (py - my)
        skew = skew + vel[2, *here] * (pz - mz)
        applied = (6.0 + reac[here]) * mid - (beside - skew)
        if k == 0:
            left = mid - (1.0 / centre) * applied
            sol[here] = (1.0 / centre) * mid
        else:
            left = res[here] - applied
            sol[here] = sol[here] + mid
        res[here] = left
        if k + 1 < ITERS:
            keep = weights[k + 1] * weights[k] * (1.0 / centre if k == 0 else 1.0)
            d[other, x, rows, mid_z] = keep * mid + (
                2.0 * weights[k + 1] / half_width
            ) * left
            return None
        return left * left

    def add(total, term):
        return total if term is None else total + term

    for side in (LOW, HIGH):
        for c in range(CHUNKS):
            x_copy(0, side, c, rhs).start()
    load_rhs.wait()

    def pack_first(x, carry):
        pack(0, x)
        return carry

    lax.fori_loop(1, nx + 1, pack_first, 0)
    open_each(0, (INNER, LOW, HIGH), "start")
    for copy in loads:
        copy.wait()

    total = jnp.zeros((ROWS, nz), jnp.float32)
    for k in range(ITERS):
        slot, other = k % 2, (k + 1) % 2
        more = k + 1 < ITERS
        open_each(slot, (INNER,), "wait_recv")
        if k > 0:
            open_each(other, (INNER,), "wait_send")

        def inner(x, total, k=k, slot=slot, other=other, more=more):
            unpack(slot, x)
            for y in range(0, ny, ROWS):
                total = add(total, block(k, x, y))
            if more:
                pack(other, x)
            return total

        total = lax.fori_loop(2, nx, inner, total)
        if more:
            open_each(other, (INNER,), "start")
        open_each(slot, (LOW, HIGH), "wait_recv")
        if k > 0:
            open_each(other, (LOW, HIGH), "wait_send")
        unpack(slot, 1)
        unpack(slot, nx)
        for c in range(CHUNKS):
            for side in (LOW, HIGH):
                x_copy(slot, side, c).wait_recv()
                if k > 0:
                    x_copy(other, side, c, rhs if k == 1 else None).wait_send()
            for x in (1, nx):
                for y in range(c * chunk, (c + 1) * chunk, ROWS):
                    total = add(total, block(k, x, y))
            if more:
                for side in (LOW, HIGH):
                    x_copy(other, side, c).start()
        if more:
            pack(other, 1)
            pack(other, nx)
            open_each(other, (LOW, HIGH), "start")

    tile = total[:, :PZ]
    for z in range(PZ, nz, PZ):
        tile = tile + total[:, z : z + PZ]
    first = 0
    for axis in (2, 1, 0):
        n, i = sizes[axis], me[axis]
        part[first + i] = tile
        copies = [
            remote(
                part.at[first + i],
                part.at[first + i],
                ps_sem.at[first + p],
                pr_sem.at[first + p],
                axis,
                lax.rem(i + p, n),
            )
            for p in range(1, n)
        ]
        for copy in copies:
            copy.start()
        for copy in copies:
            copy.wait_recv()
        tile = part[first]
        for p in range(1, n):
            tile = tile + part[first + p]
        for copy in copies:
            copy.wait_send()
        first += n
    last = (ITERS - 1) % 2
    open_each(last, (INNER, LOW, HIGH), "wait_send")
    for c in range(CHUNKS):
        for side in (LOW, HIGH):
            x_copy(last, side, c).wait_send()
    cells = nx * ny * nz * sizes[0] * sizes[1] * sizes[2]
    mean = jnp.sum(tile, keepdims=True) / cells
    norm[...] = jnp.sqrt(mean + 1e-06)


def local(sizes, right_side, reaction, velocity):
    nx, ny, nz = right_side.shape
    hbm = pl.BlockSpec(memory_space=pltpu.HBM)
    vmem = pl.BlockSpec(memory_space=pltpu.VMEM)
    dma = pltpu.SemaphoreType.DMA
    field = jax.ShapeDtypeStruct((nx, ny, nz), jnp.float32)
    sol, res, norm = pl.pallas_call(
        functools.partial(kernel, sizes),
        out_shape=(field, field, jax.ShapeDtypeStruct((1, 1), jnp.float32)),
        in_specs=[hbm] * 3,
        out_specs=(vmem, vmem, vmem),
        scratch_shapes=[
            pltpu.VMEM((2, nx + 2, ny + 2 * PY, nz + 2 * PZ), jnp.float32),
            pltpu.VMEM((nx, ny, nz), jnp.float32),
            pltpu.VMEM((3, nx, ny, nz), jnp.float32),
            pltpu.VMEM((2, 2, nx, 1, nz), jnp.float32),
            pltpu.VMEM((2, 2, nx, 1, nz), jnp.float32),
            pltpu.VMEM((sum(sizes), ROWS, PZ), jnp.float32),
            dma((5,)),
            dma((2, 2, CHUNKS)),
            dma((2, 2, CHUNKS)),
            dma((2, 2, 3)),
            dma((2, 2, 3)),
            dma((2, 2, 3)),
            dma((2, 2, 3)),
            dma((sum(sizes),)),
            dma((sum(sizes),)),
        ],
        compiler_params=pltpu.CompilerParams(
            collective_id=0,
            has_side_effects=True,
            vmem_limit_bytes=40 * 1024 * 1024,
        ),
    )(right_side, reaction, velocity)
    return sol, res, norm[0, 0]


def solution(mesh):
    sizes = tuple(mesh.shape[a] for a in AXES)
    return jax.shard_map(
        functools.partial(local, sizes),
        mesh=mesh,
        in_specs=(P("gx", "gy", "gz"), P("gx", "gy", "gz"), P(None, "gx", "gy", "gz")),
        out_specs=(P("gx", "gy", "gz"), P("gx", "gy", "gz"), P()),
        check_vma=False,
    )
```

```python
import functools
import itertools

import jax
import jax.numpy as jnp
from jax import lax
from jax.experimental import pallas as pl
from jax.experimental.pallas import tpu as pltpu
from jax.sharding import PartitionSpec as P

ITERS = 5
CHUNKS = 4
ROWS = 8

centre = 7.25
half_width = 6.75

AXES = ("gx", "gy", "gz")
PY, PZ = 8, 128
LOW, HIGH, INNER = 0, 1, 2


def chebyshev_weights(count):
    ratio_value = centre / half_width
    weights = [1.0 / ratio_value]
    for iteration in range(count):
        weights.append(1.0 / (2.0 * ratio_value - weights[-1]))
    return weights


PHASES = ((2,), (0, 1))


def phase_steps(sizes, axes):
    ranges = [range(n) if i in axes else (0,) for i, n in enumerate(sizes)]
    return [steps for steps in itertools.product(*ranges) if any(steps)]


def greeted_by(sizes):
    steps = set()
    for axes in PHASES:
        steps |= set(phase_steps(sizes, axes))
    return sorted(steps)


def phase_slots(sizes):
    return sum(len(phase_steps(sizes, axes)) + 1 for axes in PHASES)


def kernel(
    sizes,
    rhs,
    reaction,
    velocity,
    sol,
    res,
    norm,
    d,
    reac,
    vel,
    ysend,
    yrecv,
    part,
    load_sem,
    xs_sem,
    xr_sem,
    ys_sem,
    yr_sem,
    zs_sem,
    zr_sem,
    ps_sem,
    pr_sem,
):
    nx, ny, nz = rhs.shape
    weights = chebyshev_weights(ITERS)
    me = [lax.axis_index(a) for a in AXES]
    mid_y = pl.ds(PY, ny)
    mid_z = pl.ds(PZ, nz)
    chunk = ny // CHUNKS

    load_rhs = pltpu.make_async_copy(
        rhs, d.at[0, pl.ds(1, nx), mid_y, mid_z], load_sem.at[0]
    )
    load_rhs.start()
    loads = [pltpu.make_async_copy(reaction, reac, load_sem.at[1])] + [
        pltpu.make_async_copy(velocity.at[i], vel.at[i], load_sem.at[2 + i])
        for i in range(3)
    ]
    for copy in loads:
        copy.start()

    barrier = pltpu.get_barrier_semaphore()
    def shifted(steps):
        return {
            a: lax.rem(i + p, n)
            for a, n, i, p in zip(AXES, sizes, me, steps)
            if p
        }

    greeted = greeted_by(sizes)
    for steps in greeted:
        pl.semaphore_signal(
            barrier,
            inc=1,
            device_id=shifted(steps),
            device_id_type=pl.DeviceIdType.MESH,
        )

    for side, at_edge in ((LOW, me[1] == 0), (HIGH, me[1] == sizes[1] - 1)):
        @pl.when(at_edge)
        def _(side=side):
            for slot in range(2):
                yrecv[slot, side] = jnp.zeros((nx, 1, nz), jnp.float32)

    for first, at_edge in ((0, me[2] == 0), (PZ + nz, me[2] == sizes[2] - 1)):
        @pl.when(at_edge)
        def _(first=first):
            def clear(x, carry):
                for slot in range(2):
                    d[slot, x, pl.ds(PY, ny), pl.ds(first, PZ)] = jnp.zeros(
                        (ny, PZ), jnp.float32
                    )
                return carry

            lax.fori_loop(1, nx + 1, clear, 0)

    pl.semaphore_wait(barrier, len(greeted))

    def remote(src, dst, send, recv, axis, target):
        return pltpu.make_async_remote_copy(
            src_ref=src,
            dst_ref=dst,
            send_sem=send,
            recv_sem=recv,
            device_id={AXES[axis]: target},
            device_id_type=pl.DeviceIdType.MESH,
        )

    def x_copy(slot, side, c, source=None):
        n = sizes[0]
        rows = pl.ds(PY + c * chunk, chunk)
        plane, land, target = (
            (nx, 0, lax.rem(me[0] + 1, n))
            if side == LOW
            else (1, nx + 1, lax.rem(me[0] + n - 1, n))
        )
        if source is None:
            src = d.at[slot, plane, rows, mid_z]
        else:
            src = source.at[plane - 1, pl.ds(c * chunk, chunk), :]
        return remote(
            src,
            d.at[slot, land, rows, mid_z],
            xs_sem.at[slot, side, c],
            xr_sem.at[slot, side, c],
            0,
            target,
        )

    def span(group):
        return {LOW: (0, 1), HIGH: (nx - 1, 1), INNER: (1, nx - 2)}[group]

    def target_of(axis, side):
        n = sizes[axis]
        step = 1 if side == LOW else n - 1
        return lax.rem(me[axis] + step, n)

    def sends(axis, side):
        return me[axis] < sizes[axis] - 1 if side == LOW else me[axis] > 0

    def receives(axis, side):
        return me[axis] > 0 if side == LOW else me[axis] < sizes[axis] - 1

    def y_copy(slot, side, group):
        x = pl.ds(*span(group))
        return remote(
            ysend.at[slot, side, x],
            yrecv.at[slot, side, x],
            ys_sem.at[slot, side, group],
            yr_sem.at[slot, side, group],
            1,
            target_of(1, side),
        )

    def z_copy(slot, side, group):
        first, count = span(group)
        x = pl.ds(first + 1, count)
        source, land = (nz, 0) if side == LOW else (PZ, PZ + nz)
        return remote(
            d.at[slot, x, mid_y, pl.ds(source, PZ)],
            d.at[slot, x, mid_y, pl.ds(land, PZ)],
            zs_sem.at[slot, side, group],
            zr_sem.at[slot, side, group],
            2,
            target_of(2, side),
        )

    def open_each(slot, groups, act):
        for group in groups:
            for axis, copy in ((2, z_copy), (1, y_copy)):
                for side in (LOW, HIGH):
                    rule = receives if act == "wait_recv" else sends

                    @pl.when(rule(axis, side))
                    def _(copy=copy, side=side, group=group):
                        getattr(copy(slot, side, group), act)()

    def pack(slot, x):
        ysend[slot, LOW, x - 1] = d[slot, x, pl.ds(PY + ny - 1, 1), mid_z]
        ysend[slot, HIGH, x - 1] = d[slot, x, pl.ds(PY, 1), mid_z]

    def unpack(slot, x):
        d[slot, x, pl.ds(PY - 1, 1), mid_z] = yrecv[slot, LOW, x - 1]
        d[slot, x, pl.ds(PY + ny, 1), mid_z] = yrecv[slot, HIGH, x - 1]

    def block(k, x, y):
        slot, other = k % 2, (k + 1) % 2
        here = (x - 1, pl.ds(y, ROWS), slice(None))
        rows = pl.ds(PY + y, ROWS)
        mid = d[slot, x, rows, mid_z]
        px = d[slot, x + 1, rows, mid_z]
        mx = d[slot, x - 1, rows, mid_z]
        py = d[slot, x, pl.ds(PY + y + 1, ROWS), mid_z]
        my = d[slot, x, pl.ds(PY + y - 1, ROWS), mid_z]
        wide = nz + PZ
        pz = pltpu.roll(d[slot, x, rows, pl.ds(PZ, wide)], wide - 1, 1)[:, :nz]
        mz = pltpu.roll(d[slot, x, rows, pl.ds(0, wide)], 1, 1)[:, PZ:]
        beside = ((px + mx) + (py + my)) + (pz + mz)
        skew = vel[0, *here] * (px - mx) + vel[1, *here] * (py - my)
        skew = skew + vel[2, *here] * (pz - mz)
        applied = (6.0 + reac[here]) * mid - (beside - skew)
        if k == 0:
            left = mid - (1.0 / centre) * applied
            sol[here] = (1.0 / centre) * mid
        else:
            left = res[here] - applied
            sol[here] = sol[here] + mid
        res[here] = left
        if k + 1 < ITERS:
            keep = weights[k + 1] * weights[k] * (1.0 / centre if k == 0 else 1.0)
            d[other, x, rows, mid_z] = keep * mid + (
                2.0 * weights[k + 1] / half_width
            ) * left
            return None
        return left * left

    def add(total, term):
        return total if term is None else total + term

    for side in (LOW, HIGH):
        for c in range(CHUNKS):
            x_copy(0, side, c, rhs).start()
    load_rhs.wait()

    def pack_first(x, carry):
        pack(0, x)
        return carry

    lax.fori_loop(1, nx + 1, pack_first, 0)
    open_each(0, (INNER, LOW, HIGH), "start")
    for copy in loads:
        copy.wait()

    total = jnp.zeros((ROWS, nz), jnp.float32)
    for k in range(ITERS):
        slot, other = k % 2, (k + 1) % 2
        more = k + 1 < ITERS
        open_each(slot, (INNER,), "wait_recv")
        if k > 0:
            open_each(other, (INNER,), "wait_send")

        def inner(x, total, k=k, slot=slot, other=other, more=more):
            unpack(slot, x)
            for y in range(0, ny, ROWS):
                total = add(total, block(k, x, y))
            if more:
                pack(other, x)
            return total

        total = lax.fori_loop(2, nx, inner, total)
        if more:
            open_each(other, (INNER,), "start")
        open_each(slot, (LOW, HIGH), "wait_recv")
        if k > 0:
            open_each(other, (LOW, HIGH), "wait_send")
        unpack(slot, 1)
        unpack(slot, nx)
        for c in range(CHUNKS):
            for side in (LOW, HIGH):
                x_copy(slot, side, c).wait_recv()
                if k > 0:
                    x_copy(other, side, c, rhs if k == 1 else None).wait_send()
            for x in (1, nx):
                for y in range(c * chunk, (c + 1) * chunk, ROWS):
                    total = add(total, block(k, x, y))
            if more:
                for side in (LOW, HIGH):
                    x_copy(other, side, c).start()
        if more:
            pack(other, 1)
            pack(other, nx)
            open_each(other, (LOW, HIGH), "start")

    tile = total[:, :PZ]
    for z in range(PZ, nz, PZ):
        tile = tile + total[:, z : z + PZ]
    first = 0
    for axes in PHASES:
        group = phase_steps(sizes, axes)
        own = jnp.int32(0)
        for axis in axes:
            own = own * sizes[axis] + me[axis]
        part[first + own] = tile
        copies = [
            pltpu.make_async_remote_copy(
                src_ref=part.at[first + own],
                dst_ref=part.at[first + own],
                send_sem=ps_sem.at[first + p],
                recv_sem=pr_sem.at[first + p],
                device_id=shifted(steps),
                device_id_type=pl.DeviceIdType.MESH,
            )
            for p, steps in enumerate(group)
        ]
        for copy in copies:
            copy.start()
        for copy in copies:
            copy.wait_recv()
        tile = part[first]
        for p in range(1, len(group) + 1):
            tile = tile + part[first + p]
        for copy in copies:
            copy.wait_send()
        first += len(group) + 1
    last = (ITERS - 1) % 2
    open_each(last, (INNER, LOW, HIGH), "wait_send")
    for c in range(CHUNKS):
        for side in (LOW, HIGH):
            x_copy(last, side, c).wait_send()
    cells = nx * ny * nz * sizes[0] * sizes[1] * sizes[2]
    mean = jnp.sum(tile, keepdims=True) / cells
    norm[...] = jnp.sqrt(mean + 1e-06)


def local(sizes, right_side, reaction, velocity):
    nx, ny, nz = right_side.shape
    hbm = pl.BlockSpec(memory_space=pltpu.HBM)
    vmem = pl.BlockSpec(memory_space=pltpu.VMEM)
    dma = pltpu.SemaphoreType.DMA
    field = jax.ShapeDtypeStruct((nx, ny, nz), jnp.float32)
    sol, res, norm = pl.pallas_call(
        functools.partial(kernel, sizes),
        out_shape=(field, field, jax.ShapeDtypeStruct((1, 1), jnp.float32)),
        in_specs=[hbm] * 3,
        out_specs=(vmem, vmem, vmem),
        scratch_shapes=[
            pltpu.VMEM((2, nx + 2, ny + 2 * PY, nz + 2 * PZ), jnp.float32),
            pltpu.VMEM((nx, ny, nz), jnp.float32),
            pltpu.VMEM((3, nx, ny, nz), jnp.float32),
            pltpu.VMEM((2, 2, nx, 1, nz), jnp.float32),
            pltpu.VMEM((2, 2, nx, 1, nz), jnp.float32),
            pltpu.VMEM((phase_slots(sizes), ROWS, PZ), jnp.float32),
            dma((5,)),
            dma((2, 2, CHUNKS)),
            dma((2, 2, CHUNKS)),
            dma((2, 2, 3)),
            dma((2, 2, 3)),
            dma((2, 2, 3)),
            dma((2, 2, 3)),
            dma((phase_slots(sizes),)),
            dma((phase_slots(sizes),)),
        ],
        compiler_params=pltpu.CompilerParams(
            collective_id=0,
            has_side_effects=True,
            vmem_limit_bytes=40 * 1024 * 1024,
        ),
    )(
        *(
            pltpu.with_memory_space_constraint(a, pltpu.HBM)
            for a in (right_side, reaction, velocity)
        )
    )
    return sol, res, norm[0, 0]


def solution(mesh):
    sizes = tuple(mesh.shape[a] for a in AXES)
    return jax.shard_map(
        functools.partial(local, sizes),
        mesh=mesh,
        in_specs=(P("gx", "gy", "gz"), P("gx", "gy", "gz"), P(None, "gx", "gy", "gz")),
        out_specs=(P("gx", "gy", "gz"), P("gx", "gy", "gz"), P()),
        check_vma=False,
    )
```

```python
import functools
import itertools

import jax
import jax.numpy as jnp
from jax import lax
from jax.experimental import pallas as pl
from jax.experimental.pallas import tpu as pltpu
from jax.sharding import PartitionSpec as P

ITERS = 5
CHUNKS = 4
ROWS = 8

centre = 7.25
half_width = 6.75

AXES = ("gx", "gy", "gz")
PY, PZ = 8, 128
LOW, HIGH, INNER = 0, 1, 2


def chebyshev_weights(count):
    ratio_value = centre / half_width
    weights = [1.0 / ratio_value]
    for iteration in range(count):
        weights.append(1.0 / (2.0 * ratio_value - weights[-1]))
    return weights


PHASES = ((2,), (0, 1))


def phase_steps(sizes, axes):
    ranges = [range(n) if i in axes else (0,) for i, n in enumerate(sizes)]
    return [steps for steps in itertools.product(*ranges) if any(steps)]


def greeted_by(sizes):
    steps = {
        tuple(p if j == i else 0 for j in range(len(sizes)))
        for i, n in enumerate(sizes)
        for p in (1, n - 1)
    }
    if sizes[0] // 2 + sizes[1] - 1 + sizes[2] - 1 <= ITERS + 1:
        return sorted(steps)
    for axes in PHASES:
        steps |= set(phase_steps(sizes, axes))
    return sorted(steps)


def phase_slots(sizes):
    return sum(len(phase_steps(sizes, axes)) + 1 for axes in PHASES)


def kernel(
    sizes,
    rhs,
    reaction,
    velocity,
    sol,
    res,
    norm,
    d,
    reac,
    vel,
    ysend,
    yrecv,
    part,
    load_sem,
    xs_sem,
    xr_sem,
    ys_sem,
    yr_sem,
    zs_sem,
    zr_sem,
    ps_sem,
    pr_sem,
):
    nx, ny, nz = rhs.shape
    weights = chebyshev_weights(ITERS)
    me = [lax.axis_index(a) for a in AXES]
    mid_y = pl.ds(PY, ny)
    mid_z = pl.ds(PZ, nz)
    chunk = ny // CHUNKS

    load_rhs = pltpu.make_async_copy(
        rhs, d.at[0, pl.ds(1, nx), mid_y, mid_z], load_sem.at[0]
    )
    load_rhs.start()
    loads = [pltpu.make_async_copy(reaction, reac, load_sem.at[1])] + [
        pltpu.make_async_copy(velocity.at[i], vel.at[i], load_sem.at[2 + i])
        for i in range(3)
    ]
    for copy in loads:
        copy.start()

    barrier = pltpu.get_barrier_semaphore()
    def shifted(steps):
        return {
            a: lax.rem(i + p, n)
            for a, n, i, p in zip(AXES, sizes, me, steps)
            if p
        }

    greeted = greeted_by(sizes)
    for steps in greeted:
        pl.semaphore_signal(
            barrier,
            inc=1,
            device_id=shifted(steps),
            device_id_type=pl.DeviceIdType.MESH,
        )

    for side, at_edge in ((LOW, me[1] == 0), (HIGH, me[1] == sizes[1] - 1)):
        @pl.when(at_edge)
        def _(side=side):
            for slot in range(2):
                yrecv[slot, side] = jnp.zeros((nx, 1, nz), jnp.float32)

    for first, at_edge in ((0, me[2] == 0), (PZ + nz, me[2] == sizes[2] - 1)):
        @pl.when(at_edge)
        def _(first=first):
            def clear(x, carry):
                for slot in range(2):
                    d[slot, x, pl.ds(PY, ny), pl.ds(first, PZ)] = jnp.zeros(
                        (ny, PZ), jnp.float32
                    )
                return carry

            lax.fori_loop(1, nx + 1, clear, 0)

    pl.semaphore_wait(barrier, len(greeted))

    def remote(src, dst, send, recv, axis, target):
        return pltpu.make_async_remote_copy(
            src_ref=src,
            dst_ref=dst,
            send_sem=send,
            recv_sem=recv,
            device_id={AXES[axis]: target},
            device_id_type=pl.DeviceIdType.MESH,
        )

    def x_copy(slot, side, c, source=None):
        n = sizes[0]
        rows = pl.ds(PY + c * chunk, chunk)
        plane, land, target = (
            (nx, 0, lax.rem(me[0] + 1, n))
            if side == LOW
            else (1, nx + 1, lax.rem(me[0] + n - 1, n))
        )
        if source is None:
            src = d.at[slot, plane, rows, mid_z]
        else:
            src = source.at[plane - 1, pl.ds(c * chunk, chunk), :]
        return remote(
            src,
            d.at[slot, land, rows, mid_z],
            xs_sem.at[slot, side, c],
            xr_sem.at[slot, side, c],
            0,
            target,
        )

    def span(group):
        return {LOW: (0, 1), HIGH: (nx - 1, 1), INNER: (1, nx - 2)}[group]

    def target_of(axis, side):
        n = sizes[axis]
        step = 1 if side == LOW else n - 1
        return lax.rem(me[axis] + step, n)

    def sends(axis, side):
        return me[axis] < sizes[axis] - 1 if side == LOW else me[axis] > 0

    def receives(axis, side):
        return me[axis] > 0 if side == LOW else me[axis] < sizes[axis] - 1

    def y_copy(slot, side, group):
        x = pl.ds(*span(group))
        return remote(
            ysend.at[slot, side, x],
            yrecv.at[slot, side, x],
            ys_sem.at[slot, side, group],
            yr_sem.at[slot, side, group],
            1,
            target_of(1, side),
        )

    def z_copy(slot, side, group):
        first, count = span(group)
        x = pl.ds(first + 1, count)
        source, land = (nz, 0) if side == LOW else (PZ, PZ + nz)
        return remote(
            d.at[slot, x, mid_y, pl.ds(source, PZ)],
            d.at[slot, x, mid_y, pl.ds(land, PZ)],
            zs_sem.at[slot, side, group],
            zr_sem.at[slot, side, group],
            2,
            target_of(2, side),
        )

    def open_each(slot, groups, act):
        for group in groups:
            for axis, copy in ((2, z_copy), (1, y_copy)):
                for side in (LOW, HIGH):
                    rule = receives if act == "wait_recv" else sends

                    @pl.when(rule(axis, side))
                    def _(copy=copy, side=side, group=group):
                        getattr(copy(slot, side, group), act)()

    def pack(slot, x):
        ysend[slot, LOW, x - 1] = d[slot, x, pl.ds(PY + ny - 1, 1), mid_z]
        ysend[slot, HIGH, x - 1] = d[slot, x, pl.ds(PY, 1), mid_z]

    def unpack(slot, x):
        d[slot, x, pl.ds(PY - 1, 1), mid_z] = yrecv[slot, LOW, x - 1]
        d[slot, x, pl.ds(PY + ny, 1), mid_z] = yrecv[slot, HIGH, x - 1]

    def block(k, x, y):
        slot, other = k % 2, (k + 1) % 2
        here = (x - 1, pl.ds(y, ROWS), slice(None))
        rows = pl.ds(PY + y, ROWS)
        mid = d[slot, x, rows, mid_z]
        px = d[slot, x + 1, rows, mid_z]
        mx = d[slot, x - 1, rows, mid_z]
        py = d[slot, x, pl.ds(PY + y + 1, ROWS), mid_z]
        my = d[slot, x, pl.ds(PY + y - 1, ROWS), mid_z]
        wide = nz + PZ
        pz = pltpu.roll(d[slot, x, rows, pl.ds(PZ, wide)], wide - 1, 1)[:, :nz]
        mz = pltpu.roll(d[slot, x, rows, pl.ds(0, wide)], 1, 1)[:, PZ:]
        beside = ((px + mx) + (py + my)) + (pz + mz)
        skew = vel[0, *here] * (px - mx) + vel[1, *here] * (py - my)
        skew = skew + vel[2, *here] * (pz - mz)
        applied = (6.0 + reac[here]) * mid - (beside - skew)
        if k == 0:
            left = mid - (1.0 / centre) * applied
            sol[here] = (1.0 / centre) * mid
        else:
            left = res[here] - applied
            sol[here] = sol[here] + mid
        res[here] = left
        if k + 1 < ITERS:
            keep = weights[k + 1] * weights[k] * (1.0 / centre if k == 0 else 1.0)
            d[other, x, rows, mid_z] = keep * mid + (
                2.0 * weights[k + 1] / half_width
            ) * left
            return None
        return left * left

    def add(total, term):
        return total if term is None else total + term

    for side in (LOW, HIGH):
        for c in range(CHUNKS):
            x_copy(0, side, c, rhs).start()
    load_rhs.wait()

    def pack_first(x, carry):
        pack(0, x)
        return carry

    lax.fori_loop(1, nx + 1, pack_first, 0)
    open_each(0, (INNER, LOW, HIGH), "start")
    for copy in loads:
        copy.wait()

    total = jnp.zeros((ROWS, nz), jnp.float32)
    for k in range(ITERS):
        slot, other = k % 2, (k + 1) % 2
        more = k + 1 < ITERS
        open_each(slot, (INNER,), "wait_recv")
        if k > 0:
            open_each(other, (INNER,), "wait_send")

        def inner(x, total, k=k, slot=slot, other=other, more=more):
            unpack(slot, x)
            for y in range(0, ny, ROWS):
                total = add(total, block(k, x, y))
            if more:
                pack(other, x)
            return total

        total = lax.fori_loop(2, nx, inner, total)
        if more:
            open_each(other, (INNER,), "start")
        open_each(slot, (LOW, HIGH), "wait_recv")
        if k > 0:
            open_each(other, (LOW, HIGH), "wait_send")
        unpack(slot, 1)
        unpack(slot, nx)
        for c in range(CHUNKS):
            for side in (LOW, HIGH):
                x_copy(slot, side, c).wait_recv()
                if k > 0:
                    x_copy(other, side, c, rhs if k == 1 else None).wait_send()
            for x in (1, nx):
                for y in range(c * chunk, (c + 1) * chunk, ROWS):
                    total = add(total, block(k, x, y))
            if more:
                for side in (LOW, HIGH):
                    x_copy(other, side, c).start()
        if more:
            pack(other, 1)
            pack(other, nx)
            open_each(other, (LOW, HIGH), "start")

    tile = total[:, :PZ]
    for z in range(PZ, nz, PZ):
        tile = tile + total[:, z : z + PZ]
    first = 0
    for axes in PHASES:
        group = phase_steps(sizes, axes)
        own = jnp.int32(0)
        for axis in axes:
            own = own * sizes[axis] + me[axis]
        part[first + own] = tile
        copies = [
            pltpu.make_async_remote_copy(
                src_ref=part.at[first + own],
                dst_ref=part.at[first + own],
                send_sem=ps_sem.at[first + p],
                recv_sem=pr_sem.at[first + p],
                device_id=shifted(steps),
                device_id_type=pl.DeviceIdType.MESH,
            )
            for p, steps in enumerate(group)
        ]
        for copy in copies:
            copy.start()
        for copy in copies:
            copy.wait_recv()
        tile = part[first]
        for p in range(1, len(group) + 1):
            tile = tile + part[first + p]
        for copy in copies:
            copy.wait_send()
        first += len(group) + 1
    last = (ITERS - 1) % 2
    open_each(last, (INNER, LOW, HIGH), "wait_send")
    for c in range(CHUNKS):
        for side in (LOW, HIGH):
            x_copy(last, side, c).wait_send()
    cells = nx * ny * nz * sizes[0] * sizes[1] * sizes[2]
    mean = jnp.sum(tile, keepdims=True) / cells
    norm[...] = jnp.sqrt(mean + 1e-06)


def local(sizes, right_side, reaction, velocity):
    nx, ny, nz = right_side.shape
    hbm = pl.BlockSpec(memory_space=pltpu.HBM)
    vmem = pl.BlockSpec(memory_space=pltpu.VMEM)
    dma = pltpu.SemaphoreType.DMA
    field = jax.ShapeDtypeStruct((nx, ny, nz), jnp.float32)
    sol, res, norm = pl.pallas_call(
        functools.partial(kernel, sizes),
        out_shape=(field, field, jax.ShapeDtypeStruct((1, 1), jnp.float32)),
        in_specs=[hbm] * 3,
        out_specs=(vmem, vmem, vmem),
        scratch_shapes=[
            pltpu.VMEM((2, nx + 2, ny + 2 * PY, nz + 2 * PZ), jnp.float32),
            pltpu.VMEM((nx, ny, nz), jnp.float32),
            pltpu.VMEM((3, nx, ny, nz), jnp.float32),
            pltpu.VMEM((2, 2, nx, 1, nz), jnp.float32),
            pltpu.VMEM((2, 2, nx, 1, nz), jnp.float32),
            pltpu.VMEM((phase_slots(sizes), ROWS, PZ), jnp.float32),
            dma((5,)),
            dma((2, 2, CHUNKS)),
            dma((2, 2, CHUNKS)),
            dma((2, 2, 3)),
            dma((2, 2, 3)),
            dma((2, 2, 3)),
            dma((2, 2, 3)),
            dma((phase_slots(sizes),)),
            dma((phase_slots(sizes),)),
        ],
        compiler_params=pltpu.CompilerParams(
            collective_id=0,
            has_side_effects=True,
            vmem_limit_bytes=40 * 1024 * 1024,
        ),
    )(
        *(
            pltpu.with_memory_space_constraint(a, pltpu.HBM)
            for a in (right_side, reaction, velocity)
        )
    )
    return sol, res, norm[0, 0]


def solution(mesh):
    sizes = tuple(mesh.shape[a] for a in AXES)
    return jax.shard_map(
        functools.partial(local, sizes),
        mesh=mesh,
        in_specs=(P("gx", "gy", "gz"), P("gx", "gy", "gz"), P(None, "gx", "gy", "gz")),
        out_specs=(P("gx", "gy", "gz"), P("gx", "gy", "gz"), P()),
        check_vma=False,
    )
```
